16 devices in a mesh: dp: 2 (over y, z), ep: 8 (over x, core).
Axes of the slice: x: 4, y: 2, z: 1, core: 2. Of those that a mesh axis runs over, the one named last changes fastest.
The devices are a block of a 4x4x8 slice.
Arguments:
- h0: bfloat16 [16, 1024, 2048], P(('dp', 'ep')), parts along dimension 0
- idx: int32 [16, 1024, 6], P(('dp', 'ep')), parts along dimension 0
- slot: int32 [16, 1024, 6], P(('dp', 'ep')), parts along dimension 0
- ln_attn: bfloat16 [2048], replicated
- wq: bfloat16 [2048, 2048], replicated
- wk: bfloat16 [2048, 2048], replicated
- wv: bfloat16 [2048, 2048], replicated
- wo: bfloat16 [2048, 2048], replicated
- ln_ffn: bfloat16 [2048], replicated
- ws1: bfloat16 [2048, 2816], replicated
- ws3: bfloat16 [2048, 2816], replicated
- ws2: bfloat16 [2816, 2048], replicated
- ln_moe: bfloat16 [2048], replicated
- wr: bfloat16 [2048, 64], replicated
- ue1: bfloat16 [64, 2048, 1408], P('ep')
- ue3: bfloat16 [64, 2048, 1408], P('ep')
- ue2: bfloat16 [64, 1408, 2048], P('ep')
Outputs:
- output: bfloat16 [16, 1024, 2048], P(('dp', 'ep')), parts along dimension 0
There are 2 independent parts. The reference program is written for one: setup_inputs(seed, part) draws one part's arguments, and reference() takes and returns one part's arrays. A program takes and returns all parts, laid end to end along the dimension named above; an argument that names none is the same for every part.
All inputs are finite; a program needn't handle non-finite values.
Results may differ from the reference program's by a relative error of at most 0.0102599.
Values are sent between devices in bfloat16 or wider.
A program may use at most 768 MiB of HBM per device.

```python
import jax
import jax.numpy as jnp
from jax import lax

D = 2048
HEADS = 16
HEAD = 128
EXPERTS = 64
TOP = 6
FE = 1408
FS = 2816
SEQ = 1024
SEQS = 1
G = 8
CAP = 192

T = SEQS * SEQ
EPS = 1e-6


def _dot(a, b):
    return jnp.dot(a, b, preferred_element_type=jnp.float32)


def _rms(x, w):
    xf = x.astype(jnp.float32)
    r = lax.rsqrt(jnp.mean(xf * xf, axis=-1, keepdims=True) + EPS)
    return (xf * r * w.astype(jnp.float32)).astype(jnp.bfloat16)


def _rope(x):
    half = HEAD // 2
    freq = 10000.0 ** (-jnp.arange(half, dtype=jnp.float32) / half)
    ang = jnp.arange(SEQ, dtype=jnp.float32)[:, None] * freq[None, :]
    c = jnp.cos(ang)[:, None, :]
    s = jnp.sin(ang)[:, None, :]
    x1, x2 = x[..., :half], x[..., half:]
    return jnp.concatenate([x1 * c - x2 * s, x2 * c + x1 * s], axis=-1)


def _normal(key, shape, scale):
    return (jax.random.normal(key, shape, jnp.float32) * scale).astype(jnp.bfloat16)


def _scale(key):
    return jax.random.uniform(key, (D,), jnp.float32, 0.8, 1.2).astype(jnp.bfloat16)


def _expert_weight(weight_key):
    levels = jnp.sum(jax.random.randint(weight_key, (9, EXPERTS), 0, 10, jnp.int32), axis=0)
    hot_bias = 12 * (jnp.arange(EXPERTS) < EXPERTS // G).astype(jnp.int32)
    quarter = jnp.maximum(levels + hot_bias - 16, 0)
    return jnp.left_shift(4 + quarter % 4, quarter // 4).astype(jnp.int32)


def _route(route_key, weight):
    draw_rows = jax.random.bits(route_key, (T, TOP), jnp.uint32)

    def step(counts, draw_row):
        open_weight = jnp.where(counts < CAP, weight, 0).astype(jnp.int32)
        picked_list = []
        for choice in range(TOP):
            cumulative = jnp.cumsum(open_weight)
            total_weight = cumulative[-1].astype(jnp.uint32)
            target_val = (draw_row[choice] % total_weight).astype(jnp.int32)
            pick_id = jnp.searchsorted(cumulative, target_val, side='right').astype(jnp.int32)
            picked_list.append(pick_id)
            open_weight = open_weight.at[pick_id].set(0)
        chosen = jnp.stack(picked_list)
        return counts.at[chosen].add(1), (chosen, counts[chosen])

    _, (chosen, slots) = lax.scan(step, jnp.zeros((EXPERTS,), jnp.int32), draw_rows)
    return chosen.astype(jnp.int32), slots.astype(jnp.int32)


def setup_inputs(seed: int = 0, part: int = 0) -> dict:
    key = jax.random.PRNGKey(seed)
    kh, kr = jax.random.split(jax.random.fold_in(key, part))
    ks = jax.random.split(key, 15)
    hd = HEADS * HEAD
    expert_weight = _expert_weight(jax.random.fold_in(ks[14], 7))
    idx, slot = jax.vmap(lambda k: _route(k, expert_weight))(jax.random.split(kr, G))
    return {
        'h0': _normal(kh, (G * SEQS, SEQ, D), 1.0),
        'idx': idx.reshape(G * SEQS, SEQ, TOP),
        'slot': slot.reshape(G * SEQS, SEQ, TOP),
        'ln_attn': _scale(ks[0]),
        'wq': _normal(ks[1], (D, hd), 1.5 * D ** -0.5),
        'wk': _normal(ks[2], (D, hd), 1.5 * D ** -0.5),
        'wv': _normal(ks[3], (D, hd), D ** -0.5),
        'wo': _normal(ks[4], (hd, D), hd ** -0.5),
        'ln_ffn': _scale(ks[5]),
        'ws1': _normal(ks[6], (D, FS), D ** -0.5),
        'ws3': _normal(ks[7], (D, FS), D ** -0.5),
        'ws2': _normal(ks[8], (FS, D), FS ** -0.5),
        'ln_moe': _scale(ks[9]),
        'wr': _normal(ks[10], (D, EXPERTS), 1.5 * D ** -0.5),
        'ue1': _normal(ks[11], (EXPERTS, D, FE), D ** -0.5),
        'ue3': _normal(ks[12], (EXPERTS, D, FE), D ** -0.5),
        'ue2': _normal(ks[13], (EXPERTS, FE, D), 2.0 * FE ** -0.5),
    }


def reference(h0, idx, slot, ln_attn, wq, wk, wv, wo, ln_ffn, ws1, ws3, ws2, ln_moe, wr, ue1, ue3, ue2):
    nb = h0.shape[0]
    n = nb * SEQ
    x1 = _rms(h0, ln_attn)
    causal = jnp.arange(SEQ)[:, None] >= jnp.arange(SEQ)[None, :]

    def attn(xs):
        q = _rope(_dot(xs, wq).reshape(SEQ, HEADS, HEAD)).astype(jnp.bfloat16)
        k = _rope(_dot(xs, wk).reshape(SEQ, HEADS, HEAD)).astype(jnp.bfloat16)
        v = _dot(xs, wv).astype(jnp.bfloat16).reshape(SEQ, HEADS, HEAD)
        s = jnp.einsum('qhe,khe->hqk', q.astype(jnp.float32), k.astype(jnp.float32)) * HEAD ** -0.5
        p = jax.nn.softmax(jnp.where(causal[None], s, -1e30), axis=-1).astype(jnp.bfloat16)
        o = jnp.einsum('hqk,khe->qhe', p.astype(jnp.float32), v.astype(jnp.float32))
        return o.astype(jnp.bfloat16).reshape(SEQ, HEADS * HEAD)

    o = lax.map(attn, x1).reshape(n, HEADS * HEAD)
    h = h0.reshape(n, D)
    a = (h.astype(jnp.float32) + _dot(o, wo)).astype(jnp.bfloat16)
    x2 = _rms(a, ln_ffn)
    hs = (jax.nn.silu(_dot(x2, ws1)) * _dot(x2, ws3)).astype(jnp.bfloat16)
    f = _dot(hs, ws2)

    u = _rms(h, ln_moe)
    gi = idx.reshape(n, TOP)
    sl = slot.reshape(n, TOP)
    g = jax.nn.softmax(jnp.take_along_axis(_dot(u, wr), gi, axis=1), axis=-1)
    dev = jnp.arange(n, dtype=jnp.int32) // T
    pos = gi * (G * CAP) + dev[:, None] * CAP + sl
    src = jnp.full((EXPERTS * G * CAP,), n, jnp.int32).at[pos.reshape(-1)].set(
        jnp.arange(n * TOP, dtype=jnp.int32) // TOP)
    u_pad = jnp.concatenate([u, jnp.zeros((1, D), jnp.bfloat16)], axis=0)
    buf = u_pad[src].reshape(EXPERTS, G * CAP, D)

    def expert(args):
        x, w1, w3, w2 = args
        he = (jax.nn.silu(_dot(x, w1)) * _dot(x, w3)).astype(jnp.bfloat16)
        return _dot(he, w2).astype(jnp.bfloat16)

    y = lax.map(expert, (buf, ue1, ue3, ue2)).reshape(EXPERTS * G * CAP, D)
    m = jnp.sum(g[:, :, None] * y[pos].astype(jnp.float32), axis=1)
    out = a.astype(jnp.float32) + f + m
    return out.astype(jnp.bfloat16).reshape(nb, SEQ, D)
```

```python
import functools

import jax
import jax.numpy as jnp
from jax import lax
from jax.experimental import pallas as pl
from jax.experimental.pallas import tpu as pltpu
from jax.sharding import PartitionSpec as P

HEAD = 128
EPS = 1e-6
CAP_FACTOR = 2
LANE = 128
TM = 256
BLK = 64
PARTS = 2
CHUNKS = ((0, 1), (1, 2))
SUB = 8
VMEM = 63000 * 1024


def _mm(form, a, b):
    return jnp.einsum(form, a, b, preferred_element_type=jnp.float32)


def _rms(x, w):
    xf = x.astype(jnp.float32)
    r = lax.rsqrt(jnp.mean(xf * xf, axis=-1, keepdims=True) + EPS)
    return (xf * r * w.astype(jnp.float32)).astype(jnp.bfloat16)


def _qkv(h0, ln_attn, wq, wk, wv):
    x1 = _rms(h0, ln_attn)
    return (_mm('sd,de->se', x1, wq), _mm('sd,de->se', x1, wk), _mm('sd,de->se', x1, wv).astype(jnp.bfloat16))


def _heads(q, k, v):
    s, w = q.shape
    half, bq = HEAD // 2, min(256, s)
    freq = 10000.0 ** (-jnp.arange(half, dtype=jnp.float32) / half)
    ang = jnp.arange(s, dtype=jnp.float32)[:, None] * freq[None, :]
    c, sn = jnp.cos(ang), jnp.sin(ang)
    cos = jnp.concatenate([c, c], axis=1)
    sin = jnp.concatenate([-sn, sn], axis=1)

    def body(cos_ref, sin_ref, q_ref, k_ref, v_ref, o_ref):
        def rot(x):
            return (x * cos_ref[...] + pltpu.roll(x, half, 1) * sin_ref[...]).astype(jnp.bfloat16)

        qr, kr = rot(q_ref[...]), rot(k_ref[...])
        for i in range(s // bq):
            n = (i + 1) * bq
            sc = lax.dot_general(qr[i * bq:n], kr[:n], (((1,), (1,)), ((), ())),
                                 preferred_element_type=jnp.float32) * HEAD ** -0.5
            row = lax.broadcasted_iota(jnp.int32, (bq, n), 0) + i * bq
            col = lax.broadcasted_iota(jnp.int32, (bq, n), 1)
            sc = jnp.where(row >= col, sc, -1e30)
            ex = jnp.exp(sc - jnp.max(sc, axis=-1, keepdims=True))
            p = (ex / jnp.sum(ex, axis=-1, keepdims=True)).astype(jnp.bfloat16)
            o_ref[i * bq:n, :] = jnp.dot(p, v_ref[:n, :], preferred_element_type=jnp.float32).astype(jnp.bfloat16)

    col = pl.BlockSpec((s, HEAD), lambda h: (0, h))
    tab = pl.BlockSpec((s, HEAD), lambda h: (0, 0))
    return pl.pallas_call(
        body,
        out_shape=jax.ShapeDtypeStruct((s, w), jnp.bfloat16),
        grid=(w // HEAD,),
        in_specs=[tab, tab, col, col, col],
        out_specs=col,
        compiler_params=pltpu.CompilerParams(dimension_semantics=('arbitrary',), vmem_limit_bytes=VMEM),
        cost_estimate=pl.CostEstimate(flops=20_000_000_000, bytes_accessed=24_000_000, transcendentals=0),
        name='heads',
    )(cos, sin, q, k, v)


def _ffn(a, ln_ffn, ws1, ws3, ws2):
    x2 = _rms(a, ln_ffn)
    hs = (jax.nn.silu(_mm('sd,df->sf', x2, ws1)) * _mm('sd,df->sf', x2, ws3)).astype(jnp.bfloat16)
    return _mm('sf,fd->sd', hs, ws2)


def _gates(u, wr, idx_t):
    lg = _mm('td,de->et', u, wr)
    e = jnp.arange(wr.shape[1], dtype=idx_t.dtype)
    sel = jnp.sum(jnp.where(idx_t[:, None, :] == e[None, :, None], lg[None], 0.0), axis=1)
    return jax.nn.softmax(sel, axis=0)


def _tables(idx, gate, first, el, cap):
    _, g, tc = idx.shape
    eid = first + jnp.arange(el, dtype=jnp.int32)
    hit = idx[:, None] == eid[None, :, None, None]
    mask = jnp.any(hit, axis=0)
    w = jnp.sum(jnp.where(hit, gate[:, None], 0.0), axis=0)
    tri = (jnp.arange(tc)[:, None] <= jnp.arange(tc)[None, :]).astype(jnp.bfloat16)
    c = _mm('egt,tp->egp', mask.astype(jnp.bfloat16), tri).astype(jnp.int32)
    n = c[..., -1]
    p = jnp.arange(cap, dtype=jnp.int32)
    tok = jnp.sum((c[:, :, :, None] <= p).astype(jnp.int32), axis=2)
    ck = jnp.where(mask, c, 0)
    rowg = jnp.sum(jnp.where(ck[:, :, :, None] == p + 1, w[:, :, :, None], 0.0), axis=2)
    d = jnp.arange(g, dtype=jnp.int32)
    nt = g * tc
    lst = jnp.where(p < n[:, :, None], tok + d[None, :, None] * tc, nt).reshape(el, g * cap)
    lst = jnp.concatenate([lst, jnp.full((el, 8), nt, jnp.int32)], axis=1).reshape(-1)
    rowg = jnp.concatenate([rowg.reshape(el, g * cap), jnp.zeros((el, 8), jnp.float32)], axis=1).reshape(-1)
    ng = (n + 7) // 8
    ginc = jnp.sum(jnp.where(d[:, None] <= d[None, :], ng[:, :, None], 0), axis=1)
    gexc = ginc - ng
    gtot = ginc[:, -1]
    q = jnp.arange(g * cap // 8, dtype=jnp.int32)
    dq = jnp.sum((ginc[:, None, :] <= q[None, :, None]).astype(jnp.int32), axis=-1)
    gq = jnp.sum(jnp.where(dq[:, :, None] == d, gexc[:, None, :], 0), axis=-1)
    seg = jnp.where(q < gtot[:, None], dq * cap + (q[None] - gq) * 8, g * cap).reshape(-1)
    ntile = (gtot * 8 + TM - 1) // TM
    e = jnp.arange(el, dtype=jnp.int32)
    tinc = jnp.sum(jnp.where(e[:, None] <= e[None, :], ntile[:, None], 0), axis=0)
    texc = tinc - ntile
    total = jnp.maximum(tinc[-1], 1)
    i = jnp.minimum(jnp.arange(el * (g * cap // TM), dtype=jnp.int32), total - 1)
    te = jnp.minimum(jnp.sum((tinc[None, :] <= i[:, None]).astype(jnp.int32), axis=-1), el - 1)
    at = te[:, None] == e
    pick = lambda v: jnp.sum(jnp.where(at, v[None, :], 0), axis=-1)
    ti = jnp.where(i < tinc[-1], i - pick(texc), 0)
    live = ntile > 0
    order = jnp.sum(jnp.where(e[:, None] <= e[None, :], live[:, None].astype(jnp.int32), 0), axis=0)
    buf = pick(order) % 2
    after = jnp.min(jnp.where((e[None, :] > e[:, None]) & live[None, :], e[None, :], el), axis=-1)
    nxt = pick(after)
    return dict(lst=lst, rowg=rowg, seg=seg, gtot=gtot, te=te, ti=ti, buf=buf, nxt=nxt, total=total.reshape(1))


def _gather_rows(tb, u, el, rows):
    nt, kk, _ = u.shape
    nf = kk // SUB
    lstride, qm = rows + 8, rows // 8

    def body(te, ti, lst, seg, gtot, total, u_ref, x_ref, scr):
        i = pl.program_id(0)
        e = te[i]
        q0 = ti[i] * (TM // 8)
        ng = jnp.minimum(gtot[e] - q0, TM // 8)

        def group(z, _):
            for h in range(2):
                q = z * 2 + h
                s = seg[e * qm + q0 + q] + e * lstride
                for j in range(8):
                    v = u_ref[jnp.minimum(lst[s + j], nt - 1)].astype(jnp.float32)
                    at = pl.multiple_of((q * 8 + j) * SUB, SUB)
                    for f in range(nf):
                        scr[f, pl.ds(at, SUB), :] = v[f * SUB:(f + 1) * SUB]
            return 0

        def spread(lo, hi):
            for k in range(kk):
                x_ref[0, lo:hi, k * LANE:(k + 1) * LANE] = scr[
                    k // SUB, pl.ds(lo * SUB + k % SUB, hi - lo, stride=SUB), :].astype(jnp.bfloat16)

        @pl.when(i < total[0])
        def _():
            lax.fori_loop(0, (ng + 1) // 2, group, 0)
            spread(0, TM // 2)

            @pl.when(ng > TM // 16)
            def _():
                spread(TM // 2, TM)

    return pl.pallas_call(
        body,
        out_shape=jax.ShapeDtypeStruct((el, rows, kk * LANE), jnp.bfloat16),
        grid_spec=pltpu.PrefetchScalarGridSpec(
            num_scalar_prefetch=6, grid=(el * (rows // TM),),
            in_specs=[pl.BlockSpec(memory_space=pltpu.VMEM)],
            out_specs=pl.BlockSpec((1, TM, kk * LANE), lambda i, te, ti, *_: (te[i], ti[i], 0)),
            scratch_shapes=[pltpu.VMEM((nf, TM * SUB, LANE), jnp.float32)]),
        compiler_params=pltpu.CompilerParams(dimension_semantics=('arbitrary',), vmem_limit_bytes=VMEM),
        cost_estimate=pl.CostEstimate(flops=20_000_000_000, bytes_accessed=60_000_000, transcendentals=0),
        name='gather_rows',
    )(tb['te'], tb['ti'], tb['lst'], tb['seg'], tb['gtot'], tb['total'], u)


def _expert_rows(tb, x, ue1, ue3, ue2):
    el, rows, d = x.shape
    fe = ue1.shape[-1]
    kk = d // LANE
    nf = kk // SUB

    def body(te, ti, gtot, buf, nxt, total, x_ref, w1, w3, w2, y_ref, b1, b3, b2, sem):
        i = pl.program_id(0)
        e, b = te[i], buf[i]

        def copies(e, b):
            return [pltpu.make_async_copy(w.at[e], v.at[b], sem.at[b, k])
                    for k, (w, v) in enumerate(((w1, b1), (w3, b3), (w2, b2)))]

        @pl.when(i == 0)
        def _():
            for c in copies(e, b):
                c.start()

        @pl.when((ti[i] == 0) & (i < total[0]))
        def _():
            for c in copies(e, b):
                c.wait()

            @pl.when(nxt[i] < el)
            def _():
                for c in copies(nxt[i], 1 - b):
                    c.start()

        def compute(m):
            xv = x_ref[0, :m]
            h1 = jnp.dot(xv, b1[b], preferred_element_type=jnp.float32)
            h3 = jnp.dot(xv, b3[b], preferred_element_type=jnp.float32)
            he = (jax.nn.silu(h1) * h3).astype(jnp.bfloat16)
            y = jnp.dot(he, b2[b], preferred_element_type=jnp.float32)
            y = y.astype(jnp.bfloat16).astype(jnp.float32)
            for k in range(kk):
                y_ref[0, k // SUB, pl.ds(k % SUB, m, stride=SUB), :] = y[:, k * LANE:(k + 1) * LANE]

        left = gtot[e] * 8 - ti[i] * TM

        @pl.when((i < total[0]) & (left > TM // 2))
        def _():
            compute(TM)

        @pl.when((i < total[0]) & (left <= TM // 2))
        def _():
            compute(TM // 2)

    return pl.pallas_call(
        body,
        out_shape=jax.ShapeDtypeStruct((el, nf, rows * SUB, LANE), jnp.float32),
        grid_spec=pltpu.PrefetchScalarGridSpec(
            num_scalar_prefetch=6, grid=(el * (rows // TM),),
            in_specs=[pl.BlockSpec((1, TM, d), lambda i, te, ti, *_: (te[i], ti[i], 0))]
            + [pl.BlockSpec(memory_space=pl.ANY)] * 3,
            out_specs=pl.BlockSpec((1, nf, TM * SUB, LANE), lambda i, te, ti, *_: (te[i], 0, ti[i], 0)),
            scratch_shapes=[pltpu.VMEM((2, d, fe), jnp.bfloat16), pltpu.VMEM((2, d, fe), jnp.bfloat16),
                            pltpu.VMEM((2, fe, d), jnp.bfloat16), pltpu.SemaphoreType.DMA((2, 3))]),
        compiler_params=pltpu.CompilerParams(dimension_semantics=('arbitrary',), vmem_limit_bytes=VMEM),
        cost_estimate=pl.CostEstimate(flops=110_000_000_000, bytes_accessed=200_000_000, transcendentals=0),
        name='expert_rows',
    )(tb['te'], tb['ti'], tb['gtot'], tb['buf'], tb['nxt'], tb['total'], x, ue1, ue3, ue2)


def _combine_rows(tb, y, nt, kk):
    el = y.shape[0]
    nf = kk // SUB
    rows = y.shape[2] // SUB
    lstride, qm = rows + 8, rows // 8
    zb = 64

    def body(te, ti, lst, rowg, seg, gtot, total, y_ref, m_ref, acc, sem):
        i = pl.program_id(0)
        e = te[i]
        q0 = ti[i] * (TM // 8)
        ng = jnp.minimum(gtot[e] - q0, TM // 8)

        @pl.when(i == 0)
        def _():
            def zero(z, _):
                acc[pl.ds(pl.multiple_of(z * zb, zb), zb)] = jnp.zeros((zb, kk, LANE), jnp.float32)
                return 0
            lax.fori_loop(0, nt // zb, zero, 0)

        def group(z, _):
            toks, new = [], []
            for h in range(2):
                q = z * 2 + h
                s = seg[e * qm + q0 + q] + e * lstride
                for j in range(8):
                    at = pl.multiple_of((q * 8 + j) * SUB, SUB)
                    t, g = lst[s + j], rowg[s + j]
                    toks.append(t)
                    new.append([acc[t, f * SUB:(f + 1) * SUB] + g * y_ref[0, f, pl.ds(at, SUB), :] for f in range(nf)])
            for t, v in zip(toks, new):
                for f in range(nf):
                    acc[t, f * SUB:(f + 1) * SUB] = v[f]
            return 0

        @pl.when(i < total[0])
        def _():
            lax.fori_loop(0, (ng + 1) // 2, group, 0)

        @pl.when(i == pl.num_programs(0) - 1)
        def _():
            c = pltpu.make_async_copy(acc.at[pl.ds(0, nt)], m_ref, sem)
            c.start()
            c.wait()

    return pl.pallas_call(
        body,
        out_shape=jax.ShapeDtypeStruct((nt, kk, LANE), jnp.float32),
        grid_spec=pltpu.PrefetchScalarGridSpec(
            num_scalar_prefetch=7, grid=(el * (rows // TM),),
            in_specs=[pl.BlockSpec((1, nf, TM * SUB, LANE), lambda i, te, ti, *_: (te[i], 0, ti[i], 0))],
            out_specs=pl.BlockSpec(memory_space=pl.ANY),
            scratch_shapes=[pltpu.VMEM((nt + 8, kk, LANE), jnp.float32), pltpu.SemaphoreType.DMA]),
        compiler_params=pltpu.CompilerParams(dimension_semantics=('arbitrary',), vmem_limit_bytes=VMEM),
        cost_estimate=pl.CostEstimate(flops=20_000_000_000, bytes_accessed=100_000_000, transcendentals=0),
        name='combine_rows',
    )(tb['te'], tb['ti'], tb['lst'], tb['rowg'], tb['seg'], tb['gtot'], tb['total'], y)


def solution(mesh):
    g_ = mesh.shape['ep']
    rows = P(('dp', 'ep'))
    rep = P()

    def local(h0, idx, slot, ln_attn, wq, wk, wv, wo, ln_ffn, ws1, ws3, ws2, ln_moe, wr, ue1, ue3, ue2):
        b, s, d = h0.shape
        top = idx.shape[-1]
        el = ue1.shape[0]
        ne = el * g_
        t = b * s
        kk = d // LANE
        cap = CAP_FACTOR * t * top // ne
        nb = t // (BLK * PARTS)
        first = lax.axis_index('ep').astype(jnp.int32) * el

        u = _rms(h0, ln_moe).reshape(t, d)
        u4 = u.reshape(nb, PARTS, BLK, kk, LANE)
        us = []
        for lo, hi in CHUNKS:
            tc = nb * (hi - lo) * BLK
            us.append(lax.all_gather(u4[:, lo:hi].reshape(tc, kk, LANE), 'ep', axis=0))
        idx_t = idx.reshape(t, top).T
        gate = _gates(u, wr, idx_t)
        meta = lax.all_gather(jnp.concatenate([idx_t.astype(jnp.float32), gate], axis=0), 'ep', axis=1)
        meta = meta.reshape(2 * top, g_, nb, PARTS, BLK)
        tables = []
        for lo, hi in CHUNKS:
            mc = meta[:, :, :, lo:hi].reshape(2 * top, g_, -1)
            tables.append(_tables(mc[:top].astype(jnp.int32), mc[top:], first, el, cap))

        hd = h0.reshape(t, d)
        q, k, v = _qkv(hd, ln_attn, wq, wk, wv)
        q, k, v, us[0] = lax.optimization_barrier((q, k, v, us[0]))
        ms = []
        for c, (lo, hi) in enumerate(CHUNKS):
            uc, tb = us[c], tables[c]
            nt = uc.shape[0] * uc.shape[1]
            x = _gather_rows(tb, uc.reshape(nt, kk, LANE), el, g_ * cap)
            y = _expert_rows(tb, x, ue1, ue3, ue2)
            m = _combine_rows(tb, y, nt, kk)
            if c == len(CHUNKS) - 1:
                q, k, v, m = lax.optimization_barrier((q, k, v, m))
            else:
                us[c + 1], m = lax.optimization_barrier((us[c + 1], m))
            m = lax.psum_scatter(m, 'ep', scatter_dimension=0, tiled=True)
            ms.append(m.reshape(nb, hi - lo, BLK, kk, LANE))
        o = jnp.concatenate([_heads(*(z[n * s:(n + 1) * s] for z in (q, k, v))) for n in range(b)], axis=0)
        a = (hd.astype(jnp.float32) + _mm('se,ed->sd', o, wo)).astype(jnp.bfloat16)
        fo = _ffn(a, ln_ffn, ws1, ws3, ws2)
        m = jnp.concatenate(ms, axis=1).reshape(t, d)
        out = a.astype(jnp.float32) + fo + m
        return out.astype(jnp.bfloat16).reshape(b, s, d)

    specs = (rows, rows, rows) + (rep,) * 11 + (P('ep'), P('ep'), P('ep'))
    return jax.shard_map(local, mesh=mesh, in_specs=specs, out_specs=rows, check_vma=False)
```

```python
import functools

import jax
import jax.numpy as jnp
from jax import lax
from jax.experimental import pallas as pl
from jax.experimental.pallas import tpu as pltpu
from jax.sharding import PartitionSpec as P

HEAD = 128
EPS = 1e-6
CAP_FACTOR = 2
LANE = 128
TM = 256
BLK = 64
PARTS = 2
CHUNKS = ((0, 1), (1, 2))
SUB = 8
RING = 4
LOG2E = 1.4426950408889634
VMEM = 63000 * 1024


def _mm(form, a, b):
    return jnp.einsum(form, a, b, preferred_element_type=jnp.float32)


def _rms(x, w):
    xf = x.astype(jnp.float32)
    r = lax.rsqrt(jnp.mean(xf * xf, axis=-1, keepdims=True) + EPS)
    return (xf * r * w.astype(jnp.float32)).astype(jnp.bfloat16)


def _qk(h0, ln_attn, wq, wk):
    x1 = _rms(h0, ln_attn)
    return x1, _mm('sd,de->se', x1, wq), _mm('sd,de->se', x1, wk)


def _heads(q, k, v):
    s, w = q.shape
    half, bq = HEAD // 2, min(256, s)
    freq = 10000.0 ** (-jnp.arange(half, dtype=jnp.float32) / half)
    ang = jnp.arange(s, dtype=jnp.float32)[:, None] * freq[None, :]
    c, sn = jnp.cos(ang), jnp.sin(ang)
    cos = jnp.concatenate([c, c], axis=1)
    sin = jnp.concatenate([-sn, sn], axis=1)

    def body(cos_ref, sin_ref, q_ref, k_ref, v_ref, o_ref):
        def rot(x):
            return (x * cos_ref[...] + pltpu.roll(x, half, 1) * sin_ref[...]).astype(jnp.bfloat16)

        qr, kr = rot(q_ref[...]), rot(k_ref[...])
        for i in range(s // bq):
            n = (i + 1) * bq
            sc = lax.dot_general(qr[i * bq:n], kr[:n], (((1,), (1,)), ((), ())),
                                 preferred_element_type=jnp.float32)
            row = lax.broadcasted_iota(jnp.int32, (bq, bq), 0)
            col = lax.broadcasted_iota(jnp.int32, (bq, bq), 1)
            last = jnp.where(row >= col, sc[:, n - bq:], -1e30)
            sc = jnp.concatenate([sc[:, :n - bq], last], axis=1) if i else last
            ex = jnp.exp2((sc - jnp.max(sc, axis=-1, keepdims=True)) * (HEAD ** -0.5 * LOG2E))
            p = (ex * (1.0 / jnp.sum(ex, axis=-1, keepdims=True))).astype(jnp.bfloat16)
            o_ref[i * bq:n, :] = jnp.dot(p, v_ref[:n, :], preferred_element_type=jnp.float32).astype(jnp.bfloat16)

    col = pl.BlockSpec((s, HEAD), lambda h: (0, h))
    tab = pl.BlockSpec((s, HEAD), lambda h: (0, 0))
    return pl.pallas_call(
        body,
        out_shape=jax.ShapeDtypeStruct((s, w), jnp.bfloat16),
        grid=(w // HEAD,),
        in_specs=[tab, tab, col, col, col],
        out_specs=col,
        compiler_params=pltpu.CompilerParams(dimension_semantics=('arbitrary',), vmem_limit_bytes=VMEM),
        cost_estimate=pl.CostEstimate(flops=20_000_000_000, bytes_accessed=24_000_000, transcendentals=0),
        name='heads',
    )(cos, sin, q, k, v)


def _ffn(a, ln_ffn, ws1, ws3, ws2):
    x2 = _rms(a, ln_ffn)
    hs = (jax.nn.silu(_mm('sd,df->sf', x2, ws1)) * _mm('sd,df->sf', x2, ws3)).astype(jnp.bfloat16)
    return _mm('sf,fd->sd', hs, ws2)


def _gates(u, wr, idx_t):
    lg = _mm('td,de->et', u, wr)
    e = jnp.arange(wr.shape[1], dtype=idx_t.dtype)
    sel = jnp.sum(jnp.where(idx_t[:, None, :] == e[None, :, None], lg[None], 0.0), axis=1)
    return jax.nn.softmax(sel, axis=0)


def _tables(idx, gate, first, el, cap):
    _, g, tc = idx.shape
    eid = first + jnp.arange(el, dtype=jnp.int32)
    hit = idx[:, None] == eid[None, :, None, None]
    mask = jnp.any(hit, axis=0)
    w = jnp.sum(jnp.where(hit, gate[:, None], 0.0), axis=0)
    tri = (jnp.arange(tc)[:, None] <= jnp.arange(tc)[None, :]).astype(jnp.bfloat16)
    c = _mm('egt,tp->egp', mask.astype(jnp.bfloat16), tri).astype(jnp.int32)
    n = c[..., -1]
    p = jnp.arange(cap, dtype=jnp.int32)
    tok = jnp.sum((c[:, :, :, None] <= p).astype(jnp.int32), axis=2)
    ck = jnp.where(mask, c, 0)
    rowg = jnp.sum(jnp.where(ck[:, :, :, None] == p + 1, w[:, :, :, None], 0.0), axis=2)
    d = jnp.arange(g, dtype=jnp.int32)
    nt = g * tc
    lst = jnp.where(p < n[:, :, None], tok + d[None, :, None] * tc, nt).reshape(el, g * cap)
    lst = jnp.concatenate([lst, jnp.full((el, 8), nt, jnp.int32)], axis=1).reshape(-1)
    rowg = jnp.concatenate([rowg.reshape(el, g * cap), jnp.zeros((el, 8), jnp.float32)], axis=1).reshape(-1)
    ng = (n + 7) // 8
    ginc = jnp.sum(jnp.where(d[:, None] <= d[None, :], ng[:, :, None], 0), axis=1)
    gexc = ginc - ng
    gtot = ginc[:, -1]
    q = jnp.arange(g * cap // 8, dtype=jnp.int32)
    dq = jnp.sum((ginc[:, None, :] <= q[None, :, None]).astype(jnp.int32), axis=-1)
    gq = jnp.sum(jnp.where(dq[:, :, None] == d, gexc[:, None, :], 0), axis=-1)
    seg = jnp.where(q < gtot[:, None], dq * cap + (q[None] - gq) * 8, g * cap).reshape(-1)
    ntile = (gtot * 8 + TM - 1) // TM
    e = jnp.arange(el, dtype=jnp.int32)
    tinc = jnp.sum(jnp.where(e[:, None] <= e[None, :], ntile[:, None], 0), axis=0)
    texc = tinc - ntile
    total = jnp.maximum(tinc[-1], 1)
    i = jnp.minimum(jnp.arange(el * (g * cap // TM), dtype=jnp.int32), total - 1)
    te = jnp.minimum(jnp.sum((tinc[None, :] <= i[:, None]).astype(jnp.int32), axis=-1), el - 1)
    at = te[:, None] == e
    pick = lambda v: jnp.sum(jnp.where(at, v[None, :], 0), axis=-1)
    ti = jnp.where(i < tinc[-1], i - pick(texc), 0)
    live = ntile > 0
    order = jnp.sum(jnp.where(e[:, None] <= e[None, :], live[:, None].astype(jnp.int32), 0), axis=0)
    buf = pick(order) % 2
    after = jnp.min(jnp.where((e[None, :] > e[:, None]) & live[None, :], e[None, :], el), axis=-1)
    nxt = pick(after)
    return dict(lst=lst, rowg=rowg, seg=seg, gtot=gtot, te=te, ti=ti, buf=buf, nxt=nxt, total=total.reshape(1))


def _gather_rows(tb, u, el, rows):
    nt, kk, _ = u.shape
    nf = kk // SUB
    lstride, qm = rows + 8, rows // 8

    def body(te, ti, lst, seg, gtot, total, u_ref, x_ref, scr):
        i = pl.program_id(0)
        e = te[i]
        q0 = ti[i] * (TM // 8)
        ng = jnp.minimum(gtot[e] - q0, TM // 8)

        def group(z, _):
            for h in range(2):
                q = z * 2 + h
                s = seg[e * qm + q0 + q] + e * lstride
                for j in range(8):
                    v = u_ref[jnp.minimum(lst[s + j], nt - 1)].astype(jnp.float32)
                    at = pl.multiple_of((q * 8 + j) * SUB, SUB)
                    for f in range(nf):
                        scr[f, pl.ds(at, SUB), :] = v[f * SUB:(f + 1) * SUB]
            return 0

        def spread(lo, hi):
            for k in range(kk):
                x_ref[0, lo:hi, k * LANE:(k + 1) * LANE] = scr[
                    k // SUB, pl.ds(lo * SUB + k % SUB, hi - lo, stride=SUB), :].astype(jnp.bfloat16)

        @pl.when(i < total[0])
        def _():
            lax.fori_loop(0, (ng + 1) // 2, group, 0)
            spread(0, TM // 2)

            @pl.when(ng > TM // 16)
            def _():
                spread(TM // 2, TM)

    return pl.pallas_call(
        body,
        out_shape=jax.ShapeDtypeStruct((el, rows, kk * LANE), jnp.bfloat16),
        grid_spec=pltpu.PrefetchScalarGridSpec(
            num_scalar_prefetch=6, grid=(el * (rows // TM),),
            in_specs=[pl.BlockSpec(memory_space=pltpu.VMEM)],
            out_specs=pl.BlockSpec((1, TM, kk * LANE), lambda i, te, ti, *_: (te[i], ti[i], 0)),
            scratch_shapes=[pltpu.VMEM((nf, TM * SUB, LANE), jnp.float32)]),
        compiler_params=pltpu.CompilerParams(dimension_semantics=('arbitrary',), vmem_limit_bytes=VMEM),
        cost_estimate=pl.CostEstimate(flops=20_000_000_000, bytes_accessed=60_000_000, transcendentals=0),
        name='gather_rows',
    )(tb['te'], tb['ti'], tb['lst'], tb['seg'], tb['gtot'], tb['total'], u)


def _expert_rows(tb, x, ue1, ue3, ue2):
    el, rows, d = x.shape
    fe = ue1.shape[-1]
    kk = d // LANE
    nf = kk // SUB

    def body(te, ti, gtot, buf, nxt, total, x_ref, w1, w3, w2, y_ref, b1, b3, b2, sem, xb, xsem):
        i = pl.program_id(0)
        e, b = te[i], buf[i]

        def copies(e, b):
            return [pltpu.make_async_copy(w.at[e], v.at[b], sem.at[b, k])
                    for k, (w, v) in enumerate(((w1, b1), (w3, b3), (w2, b2)))]

        def tile(n):
            at = pl.ds(pl.multiple_of(ti[n] * TM, TM), TM)
            return pltpu.make_async_copy(x_ref.at[te[n], at], xb.at[n % RING], xsem.at[n % RING])

        @pl.when(i == 0)
        def _():
            for n in range(RING - 1):
                @pl.when(n < total[0])
                def _():
                    tile(n).start()

            for c in copies(e, b):
                c.start()

        @pl.when(i + RING - 1 < total[0])
        def _():
            tile(i + RING - 1).start()

        @pl.when(i < total[0])
        def _():
            tile(i).wait()

        @pl.when((ti[i] == 0) & (i < total[0]))
        def _():
            for c in copies(e, b):
                c.wait()

            @pl.when(nxt[i] < el)
            def _():
                for c in copies(nxt[i], 1 - b):
                    c.start()

        def compute(m):
            xv = xb[i % RING, :m]
            h1 = jnp.dot(xv, b1[b], preferred_element_type=jnp.float32)
            h3 = jnp.dot(xv, b3[b], preferred_element_type=jnp.float32)
            he = (jax.nn.silu(h1) * h3).astype(jnp.bfloat16)
            y = jnp.dot(he, b2[b], preferred_element_type=jnp.float32)
            y = y.astype(jnp.bfloat16).astype(jnp.float32)
            for k in range(kk):
                y_ref[0, k // SUB, pl.ds(k % SUB, m, stride=SUB), :] = y[:, k * LANE:(k + 1) * LANE]

        left = gtot[e] * 8 - ti[i] * TM

        @pl.when((i < total[0]) & (left > TM // 2))
        def _():
            compute(TM)

        @pl.when((i < total[0]) & (left <= TM // 2))
        def _():
            compute(TM // 2)

    return pl.pallas_call(
        body,
        out_shape=jax.ShapeDtypeStruct((el, nf, rows * SUB, LANE), jnp.float32),
        grid_spec=pltpu.PrefetchScalarGridSpec(
            num_scalar_prefetch=6, grid=(el * (rows // TM),),
            in_specs=[pl.BlockSpec(memory_space=pl.ANY)] * 4,
            out_specs=pl.BlockSpec((1, nf, TM * SUB, LANE), lambda i, te, ti, *_: (te[i], 0, ti[i], 0)),
            scratch_shapes=[pltpu.VMEM((2, d, fe), jnp.bfloat16), pltpu.VMEM((2, d, fe), jnp.bfloat16),
                            pltpu.VMEM((2, fe, d), jnp.bfloat16), pltpu.SemaphoreType.DMA((2, 3)),
                            pltpu.VMEM((RING, TM, d), jnp.bfloat16), pltpu.SemaphoreType.DMA((RING,))]),
        compiler_params=pltpu.CompilerParams(dimension_semantics=('arbitrary',), vmem_limit_bytes=VMEM),
        cost_estimate=pl.CostEstimate(flops=110_000_000_000, bytes_accessed=200_000_000, transcendentals=0),
        name='expert_rows',
    )(tb['te'], tb['ti'], tb['gtot'], tb['buf'], tb['nxt'], tb['total'], x, ue1, ue3, ue2)


def _combine_rows(tb, y, nt, kk):
    el = y.shape[0]
    nf = kk // SUB
    rows = y.shape[2] // SUB
    lstride, qm = rows + 8, rows // 8
    zb = 64

    def body(te, ti, lst, rowg, seg, gtot, total, y_ref, m_ref, acc, sem, yb, ysem):
        def tile(n):
            at = pl.ds(pl.multiple_of(ti[n] * TM * SUB, TM * SUB), TM * SUB)
            return pltpu.make_async_copy(y_ref.at[te[n], :, at], yb.at[n % RING], ysem.at[n % RING])

        for n in range(RING - 1):
            @pl.when(n < total[0])
            def _():
                tile(n).start()

        def zero(z, _):
            acc[pl.ds(pl.multiple_of(z * zb, zb), zb)] = jnp.zeros((zb, kk, LANE), jnp.float32)
            return 0

        lax.fori_loop(0, nt // zb, zero, 0)

        def step(i, _):
            @pl.when(i + RING - 1 < total[0])
            def _():
                tile(i + RING - 1).start()

            tile(i).wait()
            e, b = te[i], i % RING
            q0 = ti[i] * (TM // 8)
            ng = jnp.minimum(gtot[e] - q0, TM // 8)

            def group(z, _):
                toks, new = [], []
                for h in range(2):
                    q = z * 2 + h
                    s = seg[e * qm + q0 + q] + e * lstride
                    for j in range(8):
                        at = pl.multiple_of((q * 8 + j) * SUB, SUB)
                        t, g = lst[s + j], rowg[s + j]
                        toks.append(t)
                        new.append([acc[t, f * SUB:(f + 1) * SUB] + g * yb[b, f, pl.ds(at, SUB), :] for f in range(nf)])
                for t, v in zip(toks, new):
                    for f in range(nf):
                        acc[t, f * SUB:(f + 1) * SUB] = v[f]
                return 0

            lax.fori_loop(0, (ng + 1) // 2, group, 0)
            return 0

        lax.fori_loop(0, total[0], step, 0)
        c = pltpu.make_async_copy(acc.at[pl.ds(0, nt)], m_ref, sem)
        c.start()
        c.wait()

    return pl.pallas_call(
        body,
        out_shape=jax.ShapeDtypeStruct((nt, kk, LANE), jnp.float32),
        grid_spec=pltpu.PrefetchScalarGridSpec(
            num_scalar_prefetch=7, grid=(1,),
            in_specs=[pl.BlockSpec(memory_space=pl.ANY)],
            out_specs=pl.BlockSpec(memory_space=pl.ANY),
            scratch_shapes=[pltpu.VMEM((nt + 8, kk, LANE), jnp.float32), pltpu.SemaphoreType.DMA,
                            pltpu.VMEM((RING, nf, TM * SUB, LANE), jnp.float32), pltpu.SemaphoreType.DMA((RING,))]),
        compiler_params=pltpu.CompilerParams(dimension_semantics=('arbitrary',), vmem_limit_bytes=VMEM),
        cost_estimate=pl.CostEstimate(flops=20_000_000_000, bytes_accessed=100_000_000, transcendentals=0),
        name='combine_rows',
    )(tb['te'], tb['ti'], tb['lst'], tb['rowg'], tb['seg'], tb['gtot'], tb['total'], y)


def solution(mesh):
    g_ = mesh.shape['ep']
    rows = P(('dp', 'ep'))
    rep = P()

    def local(h0, idx, slot, ln_attn, wq, wk, wv, wo, ln_ffn, ws1, ws3, ws2, ln_moe, wr, ue1, ue3, ue2):
        b, s, d = h0.shape
        top = idx.shape[-1]
        el = ue1.shape[0]
        ne = el * g_
        t = b * s
        kk = d // LANE
        cap = CAP_FACTOR * t * top // ne
        nb = t // (BLK * PARTS)
        first = lax.axis_index('ep').astype(jnp.int32) * el

        u = _rms(h0, ln_moe).reshape(t, d)
        u4 = u.reshape(nb, PARTS, BLK, kk, LANE)
        us = []
        for lo, hi in CHUNKS:
            tc = nb * (hi - lo) * BLK
            us.append(lax.all_gather(u4[:, lo:hi].reshape(tc, kk, LANE), 'ep', axis=0))
        idx_t = idx.reshape(t, top).T
        gate = _gates(u, wr, idx_t)
        meta = lax.all_gather(jnp.concatenate([idx_t.astype(jnp.float32), gate], axis=0), 'ep', axis=1)
        meta = meta.reshape(2 * top, g_, nb, PARTS, BLK)
        tables = []
        for lo, hi in CHUNKS:
            mc = meta[:, :, :, lo:hi].reshape(2 * top, g_, -1)
            tables.append(_tables(mc[:top].astype(jnp.int32), mc[top:], first, el, cap))

        hd = h0.reshape(t, d)
        x1, q, k = _qk(hd, ln_attn, wq, wk)
        x1, q, k, us[0] = lax.optimization_barrier((x1, q, k, us[0]))
        ms = []
        for c, (lo, hi) in enumerate(CHUNKS):
            uc, tb = us[c], tables[c]
            nt = uc.shape[0] * uc.shape[1]
            x = _gather_rows(tb, uc.reshape(nt, kk, LANE), el, g_ * cap)
            y = _expert_rows(tb, x, ue1, ue3, ue2)
            m = _combine_rows(tb, y, nt, kk)
            if c == len(CHUNKS) - 1:
                x1, q, k, m = lax.optimization_barrier((x1, q, k, m))
            else:
                us[c + 1], m = lax.optimization_barrier((us[c + 1], m))
            m = lax.psum_scatter(m, 'ep', scatter_dimension=0, tiled=True)
            ms.append(m.reshape(nb, hi - lo, BLK, kk, LANE))
        v = _mm('sd,de->se', x1, wv).astype(jnp.bfloat16)
        o = jnp.concatenate([_heads(*(z[n * s:(n + 1) * s] for z in (q, k, v))) for n in range(b)], axis=0)
        a = (hd.astype(jnp.float32) + _mm('se,ed->sd', o, wo)).astype(jnp.bfloat16)
        fo = _ffn(a, ln_ffn, ws1, ws3, ws2)
        fo, ms[-1] = lax.optimization_barrier((fo, ms[-1]))
        m = jnp.concatenate(ms, axis=1).reshape(t, d)
        out = a.astype(jnp.float32) + fo + m
        return out.astype(jnp.bfloat16).reshape(b, s, d)

    specs = (rows, rows, rows) + (rep,) * 11 + (P('ep'), P('ep'), P('ep'))
    return jax.shard_map(local, mesh=mesh, in_specs=specs, out_specs=rows, check_vma=False)
```

```python
import functools

import jax
import jax.numpy as jnp
from jax import lax
from jax.experimental import pallas as pl
from jax.experimental.pallas import tpu as pltpu
from jax.sharding import PartitionSpec as P

HEAD = 128
EPS = 1e-6
CAP_FACTOR = 2
LANE = 128
TM = 256
BLK = 64
PARTS = 2
CHUNKS = ((0, 1), (1, 2))
SUB = 8
RING = 4
LOG2E = 1.4426950408889634
VMEM = 63000 * 1024


def _mm(form, a, b):
    return jnp.einsum(form, a, b, preferred_element_type=jnp.float32)


def _rms(x, w):
    xf = x.astype(jnp.float32)
    r = lax.rsqrt(jnp.mean(xf * xf, axis=-1, keepdims=True) + EPS)
    return (xf * r * w.astype(jnp.float32)).astype(jnp.bfloat16)


def _qk(h0, ln_attn, wq, wk):
    x1 = _rms(h0, ln_attn)
    return x1, _mm('sd,de->se', x1, wq), _mm('sd,de->se', x1, wk)


def _heads(q, k, v):
    s, w = q.shape
    half, bq = HEAD // 2, min(256, s)
    freq = 10000.0 ** (-jnp.arange(half, dtype=jnp.float32) / half)
    ang = jnp.arange(s, dtype=jnp.float32)[:, None] * freq[None, :]
    c, sn = jnp.cos(ang), jnp.sin(ang)
    cos = jnp.concatenate([c, c], axis=1)
    sin = jnp.concatenate([-sn, sn], axis=1)

    def body(cos_ref, sin_ref, q_ref, k_ref, v_ref, o_ref):
        def rot(x):
            return (x * cos_ref[...] + pltpu.roll(x, half, 1) * sin_ref[...]).astype(jnp.bfloat16)

        qr, kr = rot(q_ref[...]), rot(k_ref[...])
        for i in range(s // bq):
            n = (i + 1) * bq
            sc = lax.dot_general(qr[i * bq:n], kr[:n], (((1,), (1,)), ((), ())),
                                 preferred_element_type=jnp.float32)
            row = lax.broadcasted_iota(jnp.int32, (bq, bq), 0)
            col = lax.broadcasted_iota(jnp.int32, (bq, bq), 1)
            last = jnp.where(row >= col, sc[:, n - bq:], -1e30)
            sc = jnp.concatenate([sc[:, :n - bq], last], axis=1) if i else last
            ex = jnp.exp2((sc - jnp.max(sc, axis=-1, keepdims=True)) * (HEAD ** -0.5 * LOG2E))
            p = (ex * (1.0 / jnp.sum(ex, axis=-1, keepdims=True))).astype(jnp.bfloat16)
            o_ref[i * bq:n, :] = jnp.dot(p, v_ref[:n, :], preferred_element_type=jnp.float32).astype(jnp.bfloat16)

    col = pl.BlockSpec((s, HEAD), lambda h: (0, h))
    tab = pl.BlockSpec((s, HEAD), lambda h: (0, 0))
    return pl.pallas_call(
        body,
        out_shape=jax.ShapeDtypeStruct((s, w), jnp.bfloat16),
        grid=(w // HEAD,),
        in_specs=[tab, tab, col, col, col],
        out_specs=col,
        compiler_params=pltpu.CompilerParams(dimension_semantics=('arbitrary',), vmem_limit_bytes=VMEM),
        name='heads',
    )(cos, sin, q, k, v)


def _ffn(a, ln_ffn, ws1, ws3, ws2):
    x2 = _rms(a, ln_ffn)
    hs = (jax.nn.silu(_mm('sd,df->sf', x2, ws1)) * _mm('sd,df->sf', x2, ws3)).astype(jnp.bfloat16)
    return _mm('sf,fd->sd', hs, ws2)


def _gates(u, wr, idx_t):
    lg = _mm('td,de->et', u, wr)
    e = jnp.arange(wr.shape[1], dtype=idx_t.dtype)
    sel = jnp.sum(jnp.where(idx_t[:, None, :] == e[None, :, None], lg[None], 0.0), axis=1)
    return jax.nn.softmax(sel, axis=0)


def _tables(idx, gate, first, el, cap):
    _, g, tc = idx.shape
    eid = first + jnp.arange(el, dtype=jnp.int32)
    hit = idx[:, None] == eid[None, :, None, None]
    mask = jnp.any(hit, axis=0)
    w = jnp.sum(jnp.where(hit, gate[:, None], 0.0), axis=0)
    tri = (jnp.arange(tc)[:, None] <= jnp.arange(tc)[None, :]).astype(jnp.bfloat16)
    c = _mm('egt,tp->egp', mask.astype(jnp.bfloat16), tri).astype(jnp.int32)
    n = c[..., -1]
    p = jnp.arange(cap, dtype=jnp.int32)
    tok = jnp.sum((c[:, :, :, None] <= p).astype(jnp.int32), axis=2)
    ck = jnp.where(mask, c, 0)
    rowg = jnp.sum(jnp.where(ck[:, :, :, None] == p + 1, w[:, :, :, None], 0.0), axis=2)
    d = jnp.arange(g, dtype=jnp.int32)
    nt = g * tc
    lst = jnp.where(p < n[:, :, None], tok + d[None, :, None] * tc, nt).reshape(el, g * cap)
    lst = jnp.concatenate([lst, jnp.full((el, 8), nt, jnp.int32)], axis=1).reshape(-1)
    rowg = jnp.concatenate([rowg.reshape(el, g * cap), jnp.zeros((el, 8), jnp.float32)], axis=1).reshape(-1)
    ng = (n + 7) // 8
    ginc = jnp.sum(jnp.where(d[:, None] <= d[None, :], ng[:, :, None], 0), axis=1)
    gexc = ginc - ng
    gtot = ginc[:, -1]
    q = jnp.arange(g * cap // 8, dtype=jnp.int32)
    dq = jnp.sum((ginc[:, None, :] <= q[None, :, None]).astype(jnp.int32), axis=-1)
    gq = jnp.sum(jnp.where(dq[:, :, None] == d, gexc[:, None, :], 0), axis=-1)
    seg = jnp.where(q < gtot[:, None], dq * cap + (q[None] - gq) * 8, g * cap).reshape(-1)
    ntile = (gtot * 8 + TM - 1) // TM
    e = jnp.arange(el, dtype=jnp.int32)
    tinc = jnp.sum(jnp.where(e[:, None] <= e[None, :], ntile[:, None], 0), axis=0)
    texc = tinc - ntile
    total = jnp.maximum(tinc[-1], 1)
    i = jnp.minimum(jnp.arange(el * (g * cap // TM), dtype=jnp.int32), total - 1)
    te = jnp.minimum(jnp.sum((tinc[None, :] <= i[:, None]).astype(jnp.int32), axis=-1), el - 1)
    at = te[:, None] == e
    pick = lambda v: jnp.sum(jnp.where(at, v[None, :], 0), axis=-1)
    ti = jnp.where(i < tinc[-1], i - pick(texc), 0)
    live = ntile > 0
    order = jnp.sum(jnp.where(e[:, None] <= e[None, :], live[:, None].astype(jnp.int32), 0), axis=0)
    buf = pick(order) % 2
    after = jnp.min(jnp.where((e[None, :] > e[:, None]) & live[None, :], e[None, :], el), axis=-1)
    nxt = pick(after)
    return dict(lst=lst, rowg=rowg, seg=seg, gtot=gtot, te=te, ti=ti, buf=buf, nxt=nxt, total=total.reshape(1))


def _gather_rows(tb, u, el, rows):
    nt, kk, _ = u.shape
    nf = kk // SUB
    lstride, qm = rows + 8, rows // 8

    def body(te, ti, lst, seg, gtot, total, u_ref, x_ref, scr):
        i = pl.program_id(0)
        e = te[i]
        q0 = ti[i] * (TM // 8)
        ng = jnp.minimum(gtot[e] - q0, TM // 8)

        def group(z, _):
            for h in range(2):
                q = z * 2 + h
                s = seg[e * qm + q0 + q] + e * lstride
                for j in range(8):
                    v = u_ref[jnp.minimum(lst[s + j], nt - 1)].astype(jnp.float32)
                    at = pl.multiple_of((q * 8 + j) * SUB, SUB)
                    for f in range(nf):
                        scr[f, pl.ds(at, SUB), :] = v[f * SUB:(f + 1) * SUB]
            return 0

        def spread(lo, hi):
            for k in range(kk):
                x_ref[0, lo:hi, k * LANE:(k + 1) * LANE] = scr[
                    k // SUB, pl.ds(lo * SUB + k % SUB, hi - lo, stride=SUB), :].astype(jnp.bfloat16)

        @pl.when(i < total[0])
        def _():
            lax.fori_loop(0, (ng + 1) // 2, group, 0)
            spread(0, TM // 2)

            @pl.when(ng > TM // 16)
            def _():
                spread(TM // 2, TM)

    return pl.pallas_call(
        body,
        out_shape=jax.ShapeDtypeStruct((el, rows, kk * LANE), jnp.bfloat16),
        grid_spec=pltpu.PrefetchScalarGridSpec(
            num_scalar_prefetch=6, grid=(el * (rows // TM),),
            in_specs=[pl.BlockSpec(memory_space=pltpu.VMEM)],
            out_specs=pl.BlockSpec((1, TM, kk * LANE), lambda i, te, ti, *_: (te[i], ti[i], 0)),
            scratch_shapes=[pltpu.VMEM((nf, TM * SUB, LANE), jnp.float32)]),
        compiler_params=pltpu.CompilerParams(dimension_semantics=('arbitrary',), vmem_limit_bytes=VMEM),
        name='gather_rows',
    )(tb['te'], tb['ti'], tb['lst'], tb['seg'], tb['gtot'], tb['total'], u)


def _expert_rows(tb, x, ue1, ue3, ue2):
    el, rows, d = x.shape
    fe = ue1.shape[-1]
    kk = d // LANE
    nf = kk // SUB

    def body(te, ti, gtot, buf, nxt, total, x_ref, w1, w3, w2, y_ref, b1, b3, b2, sem):
        i = pl.program_id(0)
        e, b = te[i], buf[i]

        def copies(e, b):
            return [pltpu.make_async_copy(w.at[e], v.at[b], sem.at[b, k])
                    for k, (w, v) in enumerate(((w1, b1), (w3, b3), (w2, b2)))]

        @pl.when(i == 0)
        def _():
            for c in copies(e, b):
                c.start()

        @pl.when((ti[i] == 0) & (i < total[0]))
        def _():
            for c in copies(e, b):
                c.wait()

            @pl.when(nxt[i] < el)
            def _():
                for c in copies(nxt[i], 1 - b):
                    c.start()

        def compute(m):
            xv = x_ref[0, :m]
            h1 = jnp.dot(xv, b1[b], preferred_element_type=jnp.float32)
            h3 = jnp.dot(xv, b3[b], preferred_element_type=jnp.float32)
            he = (jax.nn.silu(h1) * h3).astype(jnp.bfloat16)
            y = jnp.dot(he, b2[b], preferred_element_type=jnp.float32)
            y = y.astype(jnp.bfloat16).astype(jnp.float32)
            for k in range(kk):
                y_ref[0, k // SUB, pl.ds(k % SUB, m, stride=SUB), :] = y[:, k * LANE:(k + 1) * LANE]

        left = gtot[e] * 8 - ti[i] * TM

        @pl.when((i < total[0]) & (left > TM // 2))
        def _():
            compute(TM)

        @pl.when((i < total[0]) & (left <= TM // 2))
        def _():
            compute(TM // 2)

    return pl.pallas_call(
        body,
        out_shape=jax.ShapeDtypeStruct((el, nf, rows * SUB, LANE), jnp.float32),
        grid_spec=pltpu.PrefetchScalarGridSpec(
            num_scalar_prefetch=6, grid=(el * (rows // TM),),
            in_specs=[pl.BlockSpec((1, TM, d), lambda i, te, ti, *_: (te[i], ti[i], 0))]
            + [pl.BlockSpec(memory_space=pl.ANY)] * 3,
            out_specs=pl.BlockSpec((1, nf, TM * SUB, LANE), lambda i, te, ti, *_: (te[i], 0, ti[i], 0)),
            scratch_shapes=[pltpu.VMEM((2, d, fe), jnp.bfloat16), pltpu.VMEM((2, d, fe), jnp.bfloat16),
                            pltpu.VMEM((2, fe, d), jnp.bfloat16), pltpu.SemaphoreType.DMA((2, 3))]),
        compiler_params=pltpu.CompilerParams(dimension_semantics=('arbitrary',), vmem_limit_bytes=VMEM),
        name='expert_rows',
    )(tb['te'], tb['ti'], tb['gtot'], tb['buf'], tb['nxt'], tb['total'], x, ue1, ue3, ue2)


def _combine_rows(tb, y, nt, kk):
    el = y.shape[0]
    nf = kk // SUB
    rows = y.shape[2] // SUB
    lstride, qm = rows + 8, rows // 8
    zb = 64

    def body(te, ti, lst, rowg, seg, gtot, total, y_ref, m_ref, acc, sem, yb, ysem):
        def tile(n):
            at = pl.ds(pl.multiple_of(ti[n] * TM * SUB, TM * SUB), TM * SUB)
            return pltpu.make_async_copy(y_ref.at[te[n], :, at], yb.at[n % RING], ysem.at[n % RING])

        for n in range(RING - 1):
            @pl.when(n < total[0])
            def _():
                tile(n).start()

        def zero(z, _):
            acc[pl.ds(pl.multiple_of(z * zb, zb), zb)] = jnp.zeros((zb, kk, LANE), jnp.float32)
            return 0

        lax.fori_loop(0, nt // zb, zero, 0)

        def step(i, _):
            @pl.when(i + RING - 1 < total[0])
            def _():
                tile(i + RING - 1).start()

            tile(i).wait()
            e, b = te[i], i % RING
            q0 = ti[i] * (TM // 8)
            ng = jnp.minimum(gtot[e] - q0, TM // 8)

            def group(z, _):
                toks, new = [], []
                for h in range(2):
                    q = z * 2 + h
                    s = seg[e * qm + q0 + q] + e * lstride
                    for j in range(8):
                        at = pl.multiple_of((q * 8 + j) * SUB, SUB)
                        t, g = lst[s + j], rowg[s + j]
                        toks.append(t)
                        new.append([acc[t, f * SUB:(f + 1) * SUB] + g * yb[b, f, pl.ds(at, SUB), :] for f in range(nf)])
                for t, v in zip(toks, new):
                    for f in range(nf):
                        acc[t, f * SUB:(f + 1) * SUB] = v[f]
                return 0

            lax.fori_loop(0, (ng + 1) // 2, group, 0)
            return 0

        lax.fori_loop(0, total[0], step, 0)
        c = pltpu.make_async_copy(acc.at[pl.ds(0, nt)], m_ref, sem)
        c.start()
        c.wait()

    return pl.pallas_call(
        body,
        out_shape=jax.ShapeDtypeStruct((nt, kk, LANE), jnp.float32),
        grid_spec=pltpu.PrefetchScalarGridSpec(
            num_scalar_prefetch=7, grid=(1,),
            in_specs=[pl.BlockSpec(memory_space=pl.ANY)],
            out_specs=pl.BlockSpec(memory_space=pl.ANY),
            scratch_shapes=[pltpu.VMEM((nt + 8, kk, LANE), jnp.float32), pltpu.SemaphoreType.DMA,
                            pltpu.VMEM((RING, nf, TM * SUB, LANE), jnp.float32), pltpu.SemaphoreType.DMA((RING,))]),
        compiler_params=pltpu.CompilerParams(dimension_semantics=('arbitrary',), vmem_limit_bytes=VMEM),
        name='combine_rows',
    )(tb['te'], tb['ti'], tb['lst'], tb['rowg'], tb['seg'], tb['gtot'], tb['total'], y)


def solution(mesh):
    g_ = mesh.shape['ep']
    rows = P(('dp', 'ep'))
    rep = P()

    def local(h0, idx, slot, ln_attn, wq, wk, wv, wo, ln_ffn, ws1, ws3, ws2, ln_moe, wr, ue1, ue3, ue2):
        b, s, d = h0.shape
        top = idx.shape[-1]
        el = ue1.shape[0]
        ne = el * g_
        t = b * s
        kk = d // LANE
        cap = CAP_FACTOR * t * top // ne
        nb = t // (BLK * PARTS)
        first = lax.axis_index('ep').astype(jnp.int32) * el

        u = _rms(h0, ln_moe).reshape(t, d)
        u4 = u.reshape(nb, PARTS, BLK, kk, LANE)
        us = []
        for lo, hi in CHUNKS:
            tc = nb * (hi - lo) * BLK
            us.append(lax.all_gather(u4[:, lo:hi].reshape(tc, kk, LANE), 'ep', axis=0))
        idx_t = idx.reshape(t, top).T
        gate = _gates(u, wr, idx_t)
        meta = lax.all_gather(jnp.concatenate([idx_t.astype(jnp.float32), gate], axis=0), 'ep', axis=1)
        meta = meta.reshape(2 * top, g_, nb, PARTS, BLK)
        tables = []
        for lo, hi in CHUNKS:
            mc = meta[:, :, :, lo:hi].reshape(2 * top, g_, -1)
            tables.append(_tables(mc[:top].astype(jnp.int32), mc[top:], first, el, cap))

        hd = h0.reshape(t, d)
        x1, q, k = _qk(hd, ln_attn, wq, wk)
        x1, q, k, us[0] = lax.optimization_barrier((x1, q, k, us[0]))
        ms = []
        for c, (lo, hi) in enumerate(CHUNKS):
            uc, tb = us[c], tables[c]
            nt = uc.shape[0] * uc.shape[1]
            x = _gather_rows(tb, uc.reshape(nt, kk, LANE), el, g_ * cap)
            y = _expert_rows(tb, x, ue1, ue3, ue2)
            m = _combine_rows(tb, y, nt, kk)
            if c == len(CHUNKS) - 1:
                x1, q, k, m = lax.optimization_barrier((x1, q, k, m))
            else:
                us[c + 1], m = lax.optimization_barrier((us[c + 1], m))
            if ms:
                ms[-1], m = lax.optimization_barrier((ms[-1], m))
            ms.append(lax.psum_scatter(m, 'ep', scatter_dimension=0, tiled=True))
        v = _mm('sd,de->se', x1, wv).astype(jnp.bfloat16)
        o = jnp.concatenate([_heads(*(z[n * s:(n + 1) * s] for z in (q, k, v))) for n in range(b)], axis=0)
        a = (hd.astype(jnp.float32) + _mm('se,ed->sd', o, wo)).astype(jnp.bfloat16)
        fo = _ffn(a, ln_ffn, ws1, ws3, ws2)
        fo, ms[-1] = lax.optimization_barrier((fo, ms[-1]))
        m = [z.reshape(nb, hi - lo, BLK, kk, LANE) for z, (lo, hi) in zip(ms, CHUNKS)]
        m = jnp.concatenate(m, axis=1).reshape(t, d)
        out = a.astype(jnp.float32) + fo + m
        return out.astype(jnp.bfloat16).reshape(b, s, d)

    specs = (rows, rows, rows) + (rep,) * 11 + (P('ep'), P('ep'), P('ep'))
    return jax.shard_map(local, mesh=mesh, in_specs=specs, out_specs=rows, check_vma=False)
```
